32 devices in a mesh: row: 8 (over z, y), col: 4 (over x, core).
Axes of the slice: x: 2, y: 2, z: 4, core: 2. Of those that a mesh axis runs over, the one named last changes fastest.
Arguments:
- lower_panel: float32 [1, 4, 512, 4096], P(None, None, 'col', 'row'), may hold values from -4 to 4, as said below
- right_side: float32 [1, 4096, 4096], P(None, 'row', 'col'), may hold values from -6 to 6
Outputs:
- solution: float32 [4, 512, 4096], P(None, None, 'col')
- updated_rhs: float32 [1, 4096, 4096], P(None, 'row', 'col')
The draws below stay inside these ranges and needn't reach their ends.
Inputs may be any that keep to these rules, and one draw needn't show every extreme that they name: `lower_panel`: L is lower triangular: entries of tiles L[g, s] with g < s and above the diagonal of L[s, s] are zero; the diagonal entries of L lie between 2 and 4.
All inputs are finite; a program needn't handle non-finite values.
Results may differ from the reference program's by a relative error of at most 0.00017.
Values sent between devices are 32-bit elements; how exact they have to be, the bound alone decides.
A program may use at most 128 MiB of HBM per device.

```python
import jax
import jax.numpy as jnp
from jax import lax

NB = 512
STEPS = 4
ROUNDS = 1
R = 4096
N_ROW = 8


def draw_lower_panel(key, part):
    first_key, second_key = jax.random.split(jax.random.fold_in(key, 11), 2)
    shape = (ROUNDS, STEPS, NB, N_ROW * NB)
    base = jax.random.truncated_normal(first_key, -4.0, 4.0, shape, jnp.float32)
    diag_values = jax.random.uniform(second_key, shape, jnp.float32, 2.0, 4.0)
    round_idx = jnp.arange(ROUNDS, dtype=jnp.int32)[:, None, None, None]
    section_idx = jnp.arange(STEPS, dtype=jnp.int32)[None, :, None, None]
    column_idx = jnp.arange(NB, dtype=jnp.int32)[None, None, :, None]
    row_pos = jnp.arange(N_ROW * NB, dtype=jnp.int32)[None, None, None, :]
    tile_idx = round_idx * N_ROW + row_pos // NB
    inner_row = row_pos % NB
    below = base * (1.0 / (STEPS * NB) ** 0.5)
    inside = jnp.where(column_idx < inner_row, base * (3.0 / NB ** 0.5), jnp.where(column_idx == inner_row, diag_values, 0.0))
    values = jnp.where(tile_idx > section_idx, below, jnp.where(tile_idx == section_idx, inside, 0.0))
    return values.astype(jnp.float32)


def level_of(stream_key, shape, pieces, low, top_value):
    factor_of = 1.0
    for axis_at, shards_of in pieces:
        draws = jax.random.uniform(jax.random.fold_in(jax.random.fold_in(stream_key, 6), axis_at), (shards_of,), jnp.float32, low / len(pieces), top_value / len(pieces))
        factor_of = factor_of * jnp.repeat(jnp.exp(draws), shape[axis_at] // shards_of).reshape((-1,) + (1,) * (len(shape) - 1 - axis_at))
    return factor_of


def bell_draw(key, shape, deviation, bound, shards=(), kind=jnp.bfloat16):
    values = deviation * jax.random.normal(key, shape, jnp.float32)
    if shards:
        values = values * level_of(key, shape, shards, -0.22, 0.18)
    return jnp.clip(values, -bound, bound).astype(kind)


def setup_inputs(seed: int = 0) -> dict:
    splits = jax.random.split(jax.random.key(seed), 3)
    return {
        "lower_panel": draw_lower_panel(jax.random.fold_in(splits[2], 71), 0),
        "right_side": bell_draw(splits[1], (ROUNDS, N_ROW * NB, R), 1.0, 6.0, ((1, 8), (2, 4)), jnp.float32),
    }


def reference(lower_panel, right_side):
    tile_count = ROUNDS * N_ROW
    rhs_tiles = right_side.reshape(tile_count, NB, right_side.shape[2])
    low_blocks = lower_panel.reshape(ROUNDS, STEPS, NB, N_ROW, NB).transpose(0, 3, 1, 4, 2).reshape(tile_count, STEPS, NB, NB)
    tile_index = jnp.arange(tile_count, dtype=jnp.int32)
    solved_list = []
    for section in range(STEPS):
        solved = lax.linalg.triangular_solve(low_blocks[section, section], rhs_tiles[section], left_side=True, lower=True)
        update = jnp.einsum('gic,cx->gix', low_blocks[:, section], solved, precision=lax.Precision.HIGHEST)
        rhs_tiles = rhs_tiles - jnp.where((tile_index > section)[:, None, None], update, jnp.float32(0.0))
        solved_list.append(solved)
    return (jnp.stack(solved_list), rhs_tiles.reshape(ROUNDS, N_ROW * NB, right_side.shape[2]))
```

```python
import functools

import jax
import jax.numpy as jnp
from jax import lax
from jax.experimental import pallas as pl
from jax.experimental.pallas import tpu as pltpu
from jax.sharding import PartitionSpec as P

MESH = pl.DeviceIdType.MESH
BASE = 32
WIDTH = 128
LAGS = (0, 1, 3, 5)


def dot(a, b):
    return jnp.dot(a, b, precision=lax.Precision.HIGHEST, preferred_element_type=jnp.float32)


def invert_unit(tile, n):
    row = lax.broadcasted_iota(jnp.int32, (n, n), 0)
    lane = lax.broadcasted_iota(jnp.int32, (n, n), 1)
    recip = 1.0 / jnp.sum(jnp.where(row == lane, tile, 0.0), axis=1, keepdims=True)
    inside = (row // BASE == lane // BASE) & (row > lane)
    fold = jnp.where(row % BASE == lane, 1.0, 0.0)
    coeff = dot(jnp.where(inside, tile * recip, 0.0), fold)
    blocks = n // BASE
    coeff = coeff.reshape(blocks, BASE, n)
    x = jnp.where(row == lane, recip, 0.0).reshape(blocks, BASE, n)
    for i in range(BASE - 1):
        x = x - coeff[:, :, i : i + 1] * x[:, i : i + 1, :]
    x = x.reshape(n, n)
    size = BASE
    while size < n:
        off = (row // size == lane // size + 1) & (row // (2 * size) == lane // (2 * size))
        x = x - dot(x, dot(jnp.where(off, tile, 0.0), x))
        size *= 2
    return x


def invert_into(low, inv):
    n = low.shape[0]
    inv[...] = jnp.zeros_like(inv)
    small = 128
    for k in range(n // small):
        at = pl.ds(k * small, small)
        inv[at, at] = invert_unit(low[at, at], small)
    size = small
    while size < n:
        for k in range(n // (2 * size)):
            top = pl.ds(2 * k * size, size)
            low_at = pl.ds((2 * k + 1) * size, size)
            inv[low_at, top] = -dot(inv[low_at, low_at], dot(low[low_at, top], inv[top, top]))
        size *= 2


def kernel(row_count, col_count, panel, rhs, sol, cur, tiles, low, inv,
           panel_send, panel_recv, hop_send, recv):
    sections, cw, n = panel.shape
    chunks = rhs.shape[1] // WIDTH
    row, col = lax.axis_index("row"), lax.axis_index("col")
    pos, plane = row // 2, row % 2
    line = row_count // 2
    partner = pos * 2 + (1 - plane)
    chips = col_count // 2
    chip, core = col // 2, col % 2
    twin = chip * 2 + (1 - core)
    up_row, down_row = jnp.minimum(row + 2, row_count - 1), jnp.maximum(row - 2, 0)
    has_up, has_down = pos < line - 1, pos > 0

    barrier = pltpu.get_barrier_semaphore()
    for step in range(1, chips):
        pl.semaphore_signal(barrier, inc=1, device_id=(row, lax.rem(chip + step, chips) * 2 + core), device_id_type=MESH)
    pl.semaphore_signal(barrier, inc=1, device_id=(row, twin), device_id_type=MESH)
    pl.semaphore_signal(barrier, inc=1, device_id=(partner, col), device_id_type=MESH)

    @pl.when(has_up)
    def _():
        pl.semaphore_signal(barrier, inc=1, device_id=(row + 2, col), device_id_type=MESH)

    @pl.when(has_down)
    def _():
        pl.semaphore_signal(barrier, inc=1, device_id=(row - 2, col), device_id_type=MESH)

    greeted = chips + 1 + jnp.where(has_up, 1, 0) + jnp.where(has_down, 1, 0)
    pl.semaphore_wait(barrier, greeted)

    def order(k):
        if k == 0:
            return jnp.where(row < sections, row, 0)
        return jnp.where((row < sections) & (k - 1 < row), k - 1, k)

    def piece(k, origin, source, target_col, slot):
        s = order(k)
        at = tiles.at[s, pl.ds(pl.multiple_of(origin * cw, cw), cw), :]
        return pltpu.make_async_remote_copy(
            src_ref=source if source is not None else at,
            dst_ref=at,
            send_sem=panel_send.at[k, slot],
            recv_sem=panel_recv.at[k, origin],
            device_id=(row, target_col),
            device_id_type=MESH,
        )

    sent = []
    for k in range(sections):
        own = panel.at[order(k)]
        for step in range(1, chips):
            c = piece(k, col, own, lax.rem(chip + step, chips) * 2 + core, step - 1)
            c.start()
            sent.append(c)
        c = piece(k, col, own, twin, chips - 1)
        c.start()
        sent.append(c)
    for s in range(sections):
        tiles[s, pl.ds(pl.multiple_of(col * cw, cw), cw), :] = panel[s]
    cur[...] = rhs[...]

    def collect(k):
        for step in range(1, chips):
            origin = lax.rem(chip + chips - step, chips) * 2 + core
            c = piece(k, origin, None, twin, chips - 1 + step)
            c.wait_recv()
            c.start()
            sent.append(c)
        for step in range(chips):
            origin = lax.rem(chip + step, chips) * 2 + (1 - core)
            piece(k, origin, None, twin, 0).wait_recv()

    collect(0)

    def columns(j):
        return pl.ds(pl.multiple_of(j * WIDTH, WIDTH), WIDTH)

    def hop(s, j, target, direction):
        at = sol.at[s, :, columns(j)]
        return pltpu.make_async_remote_copy(
            src_ref=at, dst_ref=at,
            send_sem=hop_send.at[direction, s, j],
            recv_sem=recv.at[s, j],
            device_id=(target, col), device_id_type=MESH,
        )

    def own_chunk(s, j):
        sol[s, :, columns(j)] = dot(inv[...], cur[:, columns(j)])
        hop(s, j, partner, 0).start()

        @pl.when(has_up)
        def _():
            hop(s, j, up_row, 1).start()

        @pl.when(has_down)
        def _():
            hop(s, j, down_row, 2).start()

    @pl.when(row < sections)
    def _():
        low[0] = tiles[order(0)].T
        invert_into(low.at[0], inv)

    @pl.when(row == 0)
    def _():
        @pl.loop(0, chunks)
        def _(j):
            own_chunk(0, j)

    for k in range(1, sections):
        collect(k)
    for s in range(sections):
        low[s] = tiles[s].T

    @pl.loop(0, chunks + LAGS[sections - 1])
    def _(t):
        for s in reversed(range(sections)):
            j = t - LAGS[s]

            @pl.when((j >= 0) & (j < chunks) & (row != s))
            def _(s=s, j=j):
                hop(s, j, partner, 0).wait_recv()

                @pl.when(plane == s % 2)
                def _():
                    @pl.when(has_up & (pos > s // 2))
                    def _():
                        hop(s, j, up_row, 1).start()

                    @pl.when(has_down & (pos < s // 2))
                    def _():
                        hop(s, j, down_row, 2).start()

                    hop(s, j, partner, 0).start()

                @pl.when(row > s)
                def _():
                    at = columns(j)
                    cur[:, at] = cur[:, at] - dot(low[s], sol[s, :, at])

                if s + 1 < sections:
                    @pl.when(row == s + 1)
                    def _():
                        own_chunk(s + 1, j)

    for c in sent:
        c.wait_send()
    for s in range(sections):
        @pl.when(plane == s % 2)
        def _(s=s):
            @pl.loop(0, chunks)
            def _(j):
                hop(s, j, partner, 0).wait_send()

                @pl.when(has_up & (pos >= s // 2))
                def _():
                    hop(s, j, up_row, 1).wait_send()

                @pl.when(has_down & (pos <= s // 2))
                def _():
                    hop(s, j, down_row, 2).wait_send()


def per_device(row_count, col_count, lower_panel, right_side):
    panel, rhs = lower_panel[0], right_side[0]
    sections, cw, n = panel.shape
    width = rhs.shape[1]
    chunks = width // WIDTH
    chips = col_count // 2
    vmem = pl.BlockSpec(memory_space=pltpu.VMEM)
    sol, cur = pl.pallas_call(
        functools.partial(kernel, row_count, col_count),
        out_shape=(
            jax.ShapeDtypeStruct((sections, n, width), jnp.float32),
            jax.ShapeDtypeStruct((n, width), jnp.float32),
        ),
        in_specs=[vmem, vmem],
        out_specs=(vmem, vmem),
        scratch_shapes=[
            pltpu.VMEM((sections, n, n), jnp.float32),
            pltpu.VMEM((sections, n, n), jnp.float32),
            pltpu.VMEM((n, n), jnp.float32),
            pltpu.SemaphoreType.DMA((sections, 2 * chips)),
            pltpu.SemaphoreType.DMA((sections, col_count)),
            pltpu.SemaphoreType.DMA((3, sections, chunks)),
            pltpu.SemaphoreType.DMA((sections, chunks)),
        ],
        compiler_params=pltpu.CompilerParams(
            collective_id=0, has_side_effects=True, vmem_limit_bytes=60 * 1024 * 1024
        ),
    )(panel, rhs)
    return sol, cur[None]


def solution(mesh):
    placed = (P(None, None, "col", "row"), P(None, "row", "col"))
    return jax.shard_map(
        functools.partial(per_device, mesh.shape["row"], mesh.shape["col"]),
        mesh=mesh,
        in_specs=placed,
        out_specs=(P(None, None, "col"), P(None, "row", "col")),
        check_vma=False,
    )
```
